32 devices in a mesh: tok: 4 (over y, x), din: 4 (over z), dout: 2 (over core).
Axes of the slice: x: 2, y: 2, z: 4, core: 2. Of those that a mesh axis runs over, the one named last changes fastest.
Arguments:
- inputs: bfloat16 [1024, 7168], P(('tok', 'dout'), 'din'), may hold values from -6 to 6
- out_grad: bfloat16 [1024, 9216], P(('tok', 'din'), 'dout'), may hold values from -0.1875 to 0.1875
Outputs:
- weight_grad: bfloat16 [7168, 9216], P(('din', 'tok'), 'dout')
The draws below stay inside these ranges and needn't reach their ends.
All inputs are finite; a program needn't handle non-finite values.
Results may differ from the reference program's by a relative error of at most 0.014.
Values may be sent and summed in bfloat16 or wider, within the bound.
No kernel may reach another device: no remote copies, remote signals or barrier semaphores. Data moves between devices by JAX's collectives and lax.ppermute only.
A program may use at most 64 MiB of HBM per device.

```python
import jax
import jax.numpy as jnp
from jax import lax

D = 7168
F = 9216
GROUP_ROWS = 256
TOKENS = 1024
N_TOK = 4


def spiked(drawn, rng, source, target, shards_of, factor):
    def block_of(axis_at):
        return (jnp.arange(drawn.shape[axis_at]) // (drawn.shape[axis_at] // shards_of)).reshape((-1,) + (1,) * (drawn.ndim - 1 - axis_at))

    near = jax.random.permutation(rng, shards_of)[block_of(target)]
    other_side = (block_of(target) + shards_of // 2) % shards_of
    return jnp.where((block_of(source) == near) | (block_of(source) == other_side), factor * drawn, drawn)


def block_levels(key, extent, split, smallest, largest):
    def one(position, parts):
        heights = jax.random.uniform(jax.random.fold_in(jax.random.fold_in(key, 6), position), (parts,), jnp.float32, smallest / len(split), largest / len(split))
        return jnp.repeat(jnp.exp(heights), extent[position] // parts).reshape((-1,) + (1,) * (len(extent) - position - 1))

    loudness = one(*split[0])
    for cut in split[1:]:
        loudness = loudness * one(*cut)
    return loudness


def gaussian(key, extent, scale, limit, split=(), kind=jnp.bfloat16):
    drawn = scale * jax.random.normal(key, extent, jnp.float32)
    if split:
        drawn = drawn * block_levels(key, extent, split, -0.22, 0.18)
    return jnp.clip(drawn, -limit, limit).astype(kind)


def noise_with(stream_key, dims, spread, reach, cuts, heavy, kind=jnp.bfloat16):
    result = spread * jax.random.normal(stream_key, dims, jnp.float32)
    if cuts:
        result = result * block_levels(stream_key, dims, cuts, -0.22, 0.18)
    return jnp.clip(spiked(result, jax.random.fold_in(stream_key, 3), *heavy), -reach, reach).astype(kind)


def setup_inputs(seed: int = 0) -> dict:
    seeds = jax.random.split(jax.random.key(seed), 3)
    inputs = noise_with(seeds[0], (TOKENS, D), 1.0, 6.0, ((0, 8), (1, 4)), (0, 1, 8, 2.0))
    out_grad = gaussian(seeds[1], (TOKENS, F), TOKENS ** -0.5, 0.1875, ((0, 16), (1, 2)))
    return {"inputs": inputs, "out_grad": out_grad}


def reference(inputs, out_grad):
    def add_group(total, index):
        start = (index * GROUP_ROWS).astype(jnp.int32)
        rows_in = lax.dynamic_slice_in_dim(inputs, start, GROUP_ROWS, 0)
        rows_grad = lax.dynamic_slice_in_dim(out_grad, start, GROUP_ROWS, 0)
        term = lax.dot_general(rows_in, rows_grad, (((0,), (0,)), ((), ())), preferred_element_type=jnp.float32)
        return total + term.astype(jnp.bfloat16).astype(jnp.float32), None

    total = jnp.zeros((D, F), jnp.float32)
    total, _ = lax.scan(add_group, total, jnp.arange(N_TOK, dtype=jnp.int32))
    return total.astype(jnp.bfloat16)
```

```python
import jax
import jax.numpy as jnp
from jax import lax
from jax.sharding import PartitionSpec as P

LANES = 128
SHARES = (6, 6, 4, 2)


def widths_of(total, shares):
    if total % (LANES * sum(shares)):
        return [total]
    return [total // sum(shares) * share for share in shares]


def build(n_tok, n_din, n_dout):
    rows_y = n_tok // 2
    pair = [(t, t ^ 1) for t in range(n_tok)]

    def shift_y(step):
        return [(t, ((t // 2 + step) % rows_y) * 2 + t % 2) for t in range(n_tok)]

    def shift(size, step):
        return [(i, (i + step) % size) for i in range(size)]

    small = n_din * rows_y <= 8

    def local(inputs, out_grad):
        tok, din, dout = (lax.axis_index(a) for a in ("tok", "din", "dout"))
        y, x = tok // 2, tok % 2
        rows, features = inputs.shape
        grad_rows, columns = out_grad.shape
        half = columns // 2
        pair_width = features // rows_y
        own_width = pair_width // 2
        widths = widths_of(half, SHARES if small else (1,))

        def grad_pieces(start, width):
            mine = lax.dynamic_slice_in_dim(out_grad, x * half + start, width, 1)
            theirs = lax.dynamic_slice_in_dim(out_grad, (1 - x) * half + start, width, 1)
            block = jnp.concatenate([mine, lax.ppermute(theirs, "tok", pair)], 0)
            ring = [block]
            for _ in range(n_din - 1):
                ring.append(lax.ppermute(ring[-1], "din", shift(n_din, 1)))
            if not small:
                ring = [jnp.stack(ring, 0)]
            per_y = [[p] + [lax.ppermute(p, "tok", shift_y(s)) for s in range(1, rows_y)] for p in ring]
            if small:
                return jnp.concatenate([q for p in per_y for q in p], 0)
            return jnp.stack(per_y[0], 1).reshape(-1, width)

        def input_columns():
            got = []
            for step in range(rows_y):
                target = (y + step) % rows_y
                sent = lax.dynamic_slice_in_dim(inputs, target * pair_width, pair_width, 1)
                got.append(sent if step == 0 else lax.ppermute(sent, "tok", shift_y(step)))
            got = jnp.stack(got, 0)
            got = jnp.stack([got, lax.ppermute(got, "tok", pair)], 1)
            parts = [got]
            for step in range(1, n_dout):
                parts.append(lax.ppermute(got, "dout", shift(n_dout, step)))
            got = jnp.concatenate(parts[::-1], 2)
            total_rows = rows * n_dout
            ordered = []
            for step in range(n_din):
                first = ((din - step) % n_din) * grad_rows
                at = (first - (dout + 1) * rows) % total_rows
                ordered.append(lax.dynamic_slice_in_dim(got, at, grad_rows, 2))
            got = jnp.stack(ordered, 0).reshape(-1, pair_width)
            mine = lax.dynamic_slice_in_dim(got, x * own_width, own_width, 1)
            theirs = lax.dynamic_slice_in_dim(got, (1 - x) * own_width, own_width, 1)
            return mine, theirs

        def product(left, right):
            return lax.dot_general(
                left, right, (((0,), (0,)), ((), ())), preferred_element_type=jnp.float32
            ).astype(jnp.bfloat16)

        starts = [sum(widths[:i]) for i in range(len(widths))]
        grads = [grad_pieces(s, w) for s, w in zip(starts, widths)]
        mine, theirs = input_columns()
        result = jnp.zeros((own_width, columns), jnp.bfloat16)
        for start, grad in zip(starts, grads):
            got = lax.ppermute(product(theirs, grad), "tok", pair)
            result = lax.dynamic_update_slice_in_dim(result, product(mine, grad), x * half + start, 1)
            result = lax.dynamic_update_slice_in_dim(result, got, (1 - x) * half + start, 1)
        return result

    return local


def solution(mesh):
    placed = (P(("tok", "dout"), "din"), P(("tok", "din"), "dout"))
    local = build(mesh.shape["tok"], mesh.shape["din"], mesh.shape["dout"])
    return jax.shard_map(
        local, mesh=mesh, in_specs=placed, out_specs=P(("din", "tok"), "dout"), check_vma=False
    )
```

```python
import jax
import jax.numpy as jnp
from jax import lax
from jax.sharding import PartitionSpec as P

LANES = 128
SHARES = (1,)


def widths_of(total, shares):
    if total % (LANES * sum(shares)):
        return [total]
    return [total // sum(shares) * share for share in shares]


def build(n_tok, n_din, n_dout):
    rows_y = n_tok // 2
    pair = [(t, t ^ 1) for t in range(n_tok)]

    def shift_y(step):
        return [(t, ((t // 2 + step) % rows_y) * 2 + t % 2) for t in range(n_tok)]

    def shift(size, step):
        return [(i, (i + step) % size) for i in range(size)]


    def local(inputs, out_grad):
        tok, din, dout = (lax.axis_index(a) for a in ("tok", "din", "dout"))
        y, x = tok // 2, tok % 2
        rows, features = inputs.shape
        grad_rows, columns = out_grad.shape
        half = columns // 2
        pair_width = features // rows_y
        own_width = pair_width // 2
        widths = [half]

        def grad_pieces(start, width):
            mine = lax.dynamic_slice_in_dim(out_grad, x * half + start, width, 1)
            theirs = lax.dynamic_slice_in_dim(out_grad, (1 - x) * half + start, width, 1)
            block = jnp.concatenate([mine, lax.ppermute(theirs, "tok", pair)], 0)
            ring = [block]
            for _ in range(n_din - 1):
                ring.append(lax.ppermute(ring[-1], "din", shift(n_din, 1)))
            ring = jnp.stack(ring, 0)
            per_y = [ring] + [lax.ppermute(ring, "tok", shift_y(s)) for s in range(1, rows_y)]
            return jnp.stack(per_y, 1).reshape(-1, width)

        def input_columns():
            got = []
            for step in range(rows_y):
                target = (y + step) % rows_y
                sent = lax.dynamic_slice_in_dim(inputs, target * pair_width, pair_width, 1)
                got.append(sent if step == 0 else lax.ppermute(sent, "tok", shift_y(step)))
            got = jnp.stack(got, 0)
            got = jnp.stack([got, lax.ppermute(got, "tok", pair)], 1)
            parts = [got]
            for step in range(1, n_dout):
                parts.append(lax.ppermute(got, "dout", shift(n_dout, step)))
            got = jnp.concatenate(parts[::-1], 2)
            total_rows = rows * n_dout
            ordered = []
            for step in range(n_din):
                first = ((din - step) % n_din) * grad_rows
                at = (first - (dout + 1) * rows) % total_rows
                ordered.append(lax.dynamic_slice_in_dim(got, at, grad_rows, 2))
            got = jnp.stack(ordered, 0).reshape(-1, pair_width)
            mine = lax.dynamic_slice_in_dim(got, x * own_width, own_width, 1)
            theirs = lax.dynamic_slice_in_dim(got, (1 - x) * own_width, own_width, 1)
            return mine, theirs

        def product(left, right):
            return lax.dot_general(
                left, right, (((0,), (0,)), ((), ())), preferred_element_type=jnp.float32
            ).astype(jnp.bfloat16)

        starts = [sum(widths[:i]) for i in range(len(widths))]
        grads = [grad_pieces(s, w) for s, w in zip(starts, widths)]
        mine, theirs = input_columns()
        result = jnp.zeros((own_width, columns), jnp.bfloat16)
        for start, grad in zip(starts, grads):
            got = lax.ppermute(product(theirs, grad), "tok", pair)
            result = lax.dynamic_update_slice_in_dim(result, product(mine, grad), x * half + start, 1)
            result = lax.dynamic_update_slice_in_dim(result, got, (1 - x) * half + start, 1)
        return result

    return local


def build_square(n_din, n_dout, shares):
    n_tok = 4

    def shift(size, step):
        return [(i, (i + step) % size) for i in range(size)]

    def swap(value, bit):
        return lax.ppermute(value, "tok", [(t, t ^ bit) for t in range(n_tok)])

    def local(inputs, out_grad):
        tok, din, dout = (lax.axis_index(a) for a in ("tok", "din", "dout"))
        rows, features = inputs.shape
        grad_rows, columns = out_grad.shape
        region = columns // 2
        half = region // 2
        own_width = features // n_tok
        widths = widths_of(half, shares)
        starts = [sum(widths[:i]) for i in range(len(widths))]

        def side_of(bit):
            return (tok // bit) % 2

        def column_of(bit, side, start):
            return (bit - 1) * region + side * half + start

        def grad_pieces(bit, start, width):
            mine, theirs = (
                lax.dynamic_slice_in_dim(out_grad, column_of(bit, side, start), width, 1)
                for side in (side_of(bit), 1 - side_of(bit))
            )
            block = jnp.concatenate([mine, swap(theirs, bit)], 0)
            pieces = []
            for step in range(n_din):
                pieces += [block, swap(block, 3 - bit)]
                if step < n_din - 1:
                    block = lax.ppermute(block, "din", shift(n_din, 1))
            return jnp.concatenate(pieces, 0)

        def input_columns():
            both = [inputs, swap(inputs, 2)]

            def blocks(value, order):
                return jnp.concatenate(
                    [lax.dynamic_slice_in_dim(value, (tok ^ s) * own_width, own_width, 1) for s in order], 1
                )

            kept = jnp.stack([blocks(v, (0, 1, 2)) for v in both], 0)
            sent = jnp.stack([blocks(v, (1, 0, 3)) for v in both], 0)
            got = jnp.stack([kept, swap(sent, 1)], 1)
            parts = [got]
            for step in range(1, n_dout):
                parts.append(lax.ppermute(got, "dout", shift(n_dout, step)))
            got = jnp.concatenate(parts[::-1], 2)
            ordered = []
            for step in range(n_din):
                first = ((din - step) % n_din) * grad_rows
                at = (first - (dout + 1) * rows) % (rows * n_dout)
                ordered.append(lax.dynamic_slice_in_dim(got, at, grad_rows, 2))
            return jnp.stack(ordered, 0)

        def product(left, right):
            return lax.dot_general(
                left, right, (((0,), (0,)), ((), ())), preferred_element_type=jnp.float32
            ).astype(jnp.bfloat16)

        grads = {(bit, i): grad_pieces(bit, starts[i], widths[i]) for i in range(len(widths)) for bit in (1, 2)}
        ordered = input_columns()
        lefts = {}
        for bit in (1, 2):
            turned = ordered if bit == 1 else ordered.swapaxes(1, 2)
            mine = turned[..., :own_width].reshape(-1, own_width)
            theirs = turned[..., bit * own_width : (bit + 1) * own_width].reshape(-1, own_width)
            lefts[bit] = mine, theirs
        result = jnp.zeros((own_width, columns), jnp.bfloat16)
        for (bit, i), grad in grads.items():
            mine, theirs = lefts[bit]
            got = swap(product(theirs, grad), bit)
            for value, side in ((product(mine, grad), side_of(bit)), (got, 1 - side_of(bit))):
                result = lax.dynamic_update_slice_in_dim(result, value, column_of(bit, side, starts[i]), 1)
        return result

    return local


def solution(mesh):
    placed = (P(("tok", "dout"), "din"), P(("tok", "din"), "dout"))
    sizes = mesh.shape["tok"], mesh.shape["din"], mesh.shape["dout"]
    local = build_square(*sizes[1:], SHARES) if sizes[0] == 4 and sizes[1] <= 4 else build(*sizes)
    return jax.shard_map(
        local, mesh=mesh, in_specs=placed, out_specs=P(("din", "tok"), "dout"), check_vma=False
    )
```

```python
import functools

import jax
import jax.numpy as jnp
from jax import lax
from jax.experimental import pallas as pl
from jax.experimental.pallas import tpu as pltpu
from jax.sharding import PartitionSpec as P

LANES = 128
SHARES = (1,)


def widths_of(total, shares):
    if total % (LANES * sum(shares)):
        return [total]
    return [total // sum(shares) * share for share in shares]


def build(n_tok, n_din, n_dout):
    rows_y = n_tok // 2
    pair = [(t, t ^ 1) for t in range(n_tok)]

    def shift_y(step):
        return [(t, ((t // 2 + step) % rows_y) * 2 + t % 2) for t in range(n_tok)]

    def shift(size, step):
        return [(i, (i + step) % size) for i in range(size)]


    def local(inputs, out_grad):
        tok, din, dout = (lax.axis_index(a) for a in ("tok", "din", "dout"))
        y, x = tok // 2, tok % 2
        rows, features = inputs.shape
        grad_rows, columns = out_grad.shape
        half = columns // 2
        pair_width = features // rows_y
        own_width = pair_width // 2
        widths = [half]

        def grad_pieces(start, width):
            mine = lax.dynamic_slice_in_dim(out_grad, x * half + start, width, 1)
            theirs = lax.dynamic_slice_in_dim(out_grad, (1 - x) * half + start, width, 1)
            block = jnp.concatenate([mine, lax.ppermute(theirs, "tok", pair)], 0)
            ring = [block]
            for _ in range(n_din - 1):
                ring.append(lax.ppermute(ring[-1], "din", shift(n_din, 1)))
            ring = jnp.stack(ring, 0)
            per_y = [ring] + [lax.ppermute(ring, "tok", shift_y(s)) for s in range(1, rows_y)]
            return jnp.stack(per_y, 1).reshape(-1, width)

        def input_columns():
            got = []
            for step in range(rows_y):
                target = (y + step) % rows_y
                sent = lax.dynamic_slice_in_dim(inputs, target * pair_width, pair_width, 1)
                got.append(sent if step == 0 else lax.ppermute(sent, "tok", shift_y(step)))
            got = jnp.stack(got, 0)
            got = jnp.stack([got, lax.ppermute(got, "tok", pair)], 1)
            parts = [got]
            for step in range(1, n_dout):
                parts.append(lax.ppermute(got, "dout", shift(n_dout, step)))
            got = jnp.concatenate(parts[::-1], 2)
            total_rows = rows * n_dout
            ordered = []
            for step in range(n_din):
                first = ((din - step) % n_din) * grad_rows
                at = (first - (dout + 1) * rows) % total_rows
                ordered.append(lax.dynamic_slice_in_dim(got, at, grad_rows, 2))
            got = jnp.stack(ordered, 0).reshape(-1, pair_width)
            mine = lax.dynamic_slice_in_dim(got, x * own_width, own_width, 1)
            theirs = lax.dynamic_slice_in_dim(got, (1 - x) * own_width, own_width, 1)
            return mine, theirs

        def product(left, right):
            return lax.dot_general(
                left, right, (((0,), (0,)), ((), ())), preferred_element_type=jnp.float32
            ).astype(jnp.bfloat16)

        starts = [sum(widths[:i]) for i in range(len(widths))]
        grads = [grad_pieces(s, w) for s, w in zip(starts, widths)]
        mine, theirs = input_columns()
        result = jnp.zeros((own_width, columns), jnp.bfloat16)
        for start, grad in zip(starts, grads):
            got = lax.ppermute(product(theirs, grad), "tok", pair)
            result = lax.dynamic_update_slice_in_dim(result, product(mine, grad), x * half + start, 1)
            result = lax.dynamic_update_slice_in_dim(result, got, (1 - x) * half + start, 1)
        return result

    return local


def multiply_kernel(bit, block, n_din, n_dout, sizes, place_ref, *refs):
    rows, grad_rows = sizes
    n_left = 3 * n_dout
    lefts, grads = refs[:n_left], refs[n_left : n_left + 2 * n_din]
    out_ref, left, right, sems = refs[n_left + 2 * n_din :]
    tok, din, dout = place_ref[0], place_ref[1], place_ref[2]
    group = rows * n_dout
    copies = []

    def copy(source, target):
        copies.append(pltpu.make_async_copy(source, target, sems.at[len(copies)]))
        copies[-1].start()

    for step in range(n_din):
        first = ((din + n_din - step) % n_din) * grad_rows
        part = (dout + n_dout - first // rows) % n_dout
        for other in range(2):
            for this in range(2):
                group_at = 2 * other + this if bit == 1 else other + 2 * this
                at = pl.multiple_of(group_at * group + part * rows + first % rows, grad_rows)
                copy(grads[2 * step + other].at[pl.ds(this * grad_rows, grad_rows)], right.at[pl.ds(at, grad_rows)])
    for part in range(n_dout):
        own, over, across = lefts[3 * part : 3 * part + 3]
        sources = own.at[tok ^ block], across.at[0, block], over.at[tok ^ block], across.at[1, block]
        for group_at, source in enumerate(sources):
            copy(source, left.at[:, pl.ds(group_at * group + part * rows, rows)])
    for item in copies:
        item.wait()
    width = out_ref.shape[1]
    tile = max(t for t in (384, 256, 128, width) if width % t == 0 and t <= max(384, width % 128 and width))
    for at in range(0, width, tile):
        out_ref[:, at : at + tile] = jnp.dot(
            left[...], right[:, at : at + tile], preferred_element_type=jnp.float32
        ).astype(out_ref.dtype)


def build_square(n_din, n_dout, shares):
    n_tok = 4

    def shift(size, step):
        return [(i, (i + step) % size) for i in range(size)]

    def swap(value, bit):
        return lax.ppermute(value, "tok", [(t, t ^ bit) for t in range(n_tok)])

    def local(inputs, out_grad):
        tok, din, dout = (lax.axis_index(a) for a in ("tok", "din", "dout"))
        rows, features = inputs.shape
        grad_rows, columns = out_grad.shape
        region = columns // 2
        half = region // 2
        own_width = features // n_tok
        tokens = n_tok * n_dout * rows
        widths = widths_of(half, shares)
        starts = [sum(widths[:i]) for i in range(len(widths))]
        place = jnp.stack([tok, din, dout]).astype(jnp.int32)

        def side_of(bit):
            return (tok // bit) % 2

        def column_of(bit, side, start):
            return (bit - 1) * region + side * half + start

        def grad_pieces(bit, start, width):
            mine, theirs = (
                lax.dynamic_slice_in_dim(out_grad, column_of(bit, side, start), width, 1)
                for side in (side_of(bit), 1 - side_of(bit))
            )
            piece = jnp.concatenate([mine, swap(theirs, bit)], 0)
            pieces = []
            for step in range(n_din):
                pieces += [piece, swap(piece, 3 - bit)]
                if step < n_din - 1:
                    piece = lax.ppermute(piece, "din", shift(n_din, 1))
            return pieces

        def left_pieces():
            own = inputs.T.reshape(n_tok, own_width, rows)
            over = swap(own, 2)
            sent = jnp.stack(
                [
                    jnp.concatenate([lax.dynamic_slice_in_dim(v, tok ^ s, 1, 0) for s in (1, 0, 3)], 0)
                    for v in (own, over)
                ],
                0,
            )
            near = [own, over, swap(sent, 1)]
            pieces = list(near)
            for step in range(1, n_dout):
                pieces += [lax.ppermute(v, "dout", shift(n_dout, step)) for v in near]
            return pieces

        def product(bit, block, lefts, grads):
            width = grads[0].shape[1]
            anywhere = pl.BlockSpec(memory_space=pl.ANY)
            return pl.pallas_call(
                functools.partial(multiply_kernel, bit, block, n_din, n_dout, (rows, grad_rows)),
                out_shape=jax.ShapeDtypeStruct((own_width, width), jnp.bfloat16),
                in_specs=[pl.BlockSpec(memory_space=pltpu.SMEM)] + [anywhere] * (len(lefts) + len(grads)),
                out_specs=pl.BlockSpec(memory_space=pltpu.VMEM),
                scratch_shapes=[
                    pltpu.VMEM((own_width, tokens), jnp.bfloat16),
                    pltpu.VMEM((tokens, width), jnp.bfloat16),
                    pltpu.SemaphoreType.DMA((4 * n_din + 4 * n_dout,)),
                ],
                compiler_params=pltpu.CompilerParams(vmem_limit_bytes=24 * 2**20),
                cost_estimate=pl.CostEstimate(
                    flops=2 * own_width * tokens * width,
                    bytes_accessed=2 * (tokens * (own_width + width) + own_width * width),
                    transcendentals=0,
                ),
                name=f"multiply_{bit}_{block}",
            )(place, *lefts, *grads)

        grads = {(bit, i): grad_pieces(bit, starts[i], widths[i]) for i in range(len(widths)) for bit in (1, 2)}
        lefts = left_pieces()
        result = jnp.zeros((own_width, columns), jnp.bfloat16)
        for (bit, i), grad in grads.items():
            got = swap(product(bit, bit, lefts, grad), bit)
            for value, side in ((product(bit, 0, lefts, grad), side_of(bit)), (got, 1 - side_of(bit))):
                result = lax.dynamic_update_slice_in_dim(result, value, column_of(bit, side, starts[i]), 1)
        return result

    return local


def solution(mesh):
    placed = (P(("tok", "dout"), "din"), P(("tok", "din"), "dout"))
    sizes = mesh.shape["tok"], mesh.shape["din"], mesh.shape["dout"]
    local = build_square(*sizes[1:], SHARES) if sizes[0] == 4 and sizes[1] <= 4 else build(*sizes)
    return jax.shard_map(
        local, mesh=mesh, in_specs=placed, out_specs=P(("din", "tok"), "dout"), check_vma=False
    )
```
